32 devices in a mesh: section: 2 (over y), dp: 16 (over z, x, core).
Axes of the slice: x: 2, y: 2, z: 4, core: 2. Of those that a mesh axis runs over, the one named last changes fastest.
Arguments:
- residuals: float32 [8, 128, 4096], P('section', 'dp'), may hold values from -100 to 100, as said below
- owners: int32 [32], replicated, may hold values from 0 to 31, each once
Outputs:
- harvest: bfloat16 [128, 8, 4096], P(('section', 'dp'))
The draws below stay inside these ranges and needn't reach their ends.
Inputs may be any that keep to these rules, and one draw needn't show every extreme that they name: `owners`: a permutation of the block numbers. `residuals`: real-valued activations.
All inputs are finite; a program needn't handle non-finite values.
Results may differ from the reference program's by a relative error of at most 0.0004.
Values may be sent and summed in bfloat16 or wider, within the bound.
A program may use at most 64 MiB of HBM per device.

```python
import math
import jax
import jax.numpy as jnp
from jax import lax

D = 4096
BLOCK = 4
LAYERS = 8
TOK_DEV = 8
TOKENS = 128
BLOCKS = 32


def draw_residuals(key, part):
    noise_key = jax.random.fold_in(key, 11)
    shard_key = jax.random.fold_in(key, 12)
    token_key = jax.random.fold_in(key, 13)
    offset_key = jax.random.fold_in(key, 14)
    shard_count = TOKENS // TOK_DEV
    base_noise = jax.random.normal(noise_key, (LAYERS, TOKENS, D), jnp.float32)
    log_low = math.log(0.3)
    log_high = math.log(3.0)
    shard_scale = jnp.exp(jax.random.uniform(shard_key, (LAYERS, shard_count, 1, 1), jnp.float32, log_low, log_high))
    token_scale = jax.random.uniform(token_key, (LAYERS, TOKENS, 1), jnp.float32, 0.5, 1.5)
    offset = 2.0 * jax.random.normal(offset_key, (LAYERS, TOKENS, 1), jnp.float32)
    scaled_rows = base_noise.reshape(LAYERS, shard_count, TOK_DEV, D) * shard_scale
    return jnp.clip(scaled_rows.reshape(LAYERS, TOKENS, D) * token_scale + offset, -100.0, 100.0)


def setup_inputs(seed: int = 0) -> dict:
    key_list = jax.random.split(jax.random.key(seed), 3)
    return {
        "residuals": draw_residuals(jax.random.fold_in(key_list[2], 71), 0),
        "owners": jax.random.permutation(key_list[1], BLOCKS).astype(jnp.int32),
    }


def reference(residuals, owners):

    def normalize_layer(layer_rows):
        centered = layer_rows - lax.optimization_barrier(jnp.mean(layer_rows, axis=1, keepdims=True))
        energy = jnp.sum(centered * centered)
        layer_scale = 1.0 / jnp.sqrt(energy / (TOKENS * D) + 1.0)
        return (centered * layer_scale).astype(jnp.bfloat16)
    normed = lax.map(normalize_layer, residuals)
    inverse = jnp.zeros((BLOCKS,), jnp.int32).at[owners.astype(jnp.int32)].set(jnp.arange(BLOCKS, dtype=jnp.int32))
    blocked = normed.reshape(LAYERS, BLOCKS, BLOCK, D)[:, inverse]
    return blocked.transpose(1, 2, 0, 3).reshape(TOKENS, LAYERS, D)
```

```python
import functools

import jax
import jax.numpy as jnp
from jax import lax
from jax.experimental import pallas as pl
from jax.experimental.pallas import tpu as pltpu
from jax.sharding import PartitionSpec as P

MESH = pl.DeviceIdType.MESH
LANES = 128
SUBLANES = 8


def harvest_kernel(sections, groups, x_hbm, owners, out_ref, inverse, xv, centered, part, parts, s1, s2, r2,
                   x_sem, e_send, e_recv, send1, recv1, send2, recv2, *r1):
    layers, tokens, features = x_hbm.shape
    chunks, blocks, rows, _ = s1.shape
    width = features // groups
    block_len = rows // layers
    per_dev = tokens // block_len
    devices = sections * groups
    section, group = lax.axis_index("section"), lax.axis_index("dp")
    me = section * groups + group

    load = pltpu.make_async_copy(x_hbm, xv, x_sem)
    load.start()
    barrier = pltpu.get_barrier_semaphore()

    def peer_of(k):
        return lax.rem(group + k, groups)

    for k in range(1, groups):
        pl.semaphore_signal(barrier, inc=1, device_id=(section, peer_of(k)), device_id_type=MESH)
    for k in range(1, sections):
        pl.semaphore_signal(barrier, inc=1, device_id=(lax.rem(section + k, sections), group), device_id_type=MESH)

    load.wait()
    per_tile = SUBLANES // layers
    acc = jnp.zeros((SUBLANES, LANES), jnp.float32)
    for g in range(tokens // per_tile):
        x8 = jnp.concatenate([xv[:, g * per_tile + i, :] for i in range(per_tile)], axis=0)
        c = x8 - jnp.sum(x8, axis=1, keepdims=True) * (1.0 / features)
        centered[g * SUBLANES:(g + 1) * SUBLANES, :] = c
        sq = c * c
        for f in range(features // LANES):
            acc = acc + sq[:, f * LANES:(f + 1) * LANES]
    part[...] = acc
    parts[group] = acc

    pl.semaphore_wait(barrier, groups + sections - 2)
    for k in range(1, groups):
        pltpu.make_async_remote_copy(
            src_ref=part, dst_ref=parts.at[group], send_sem=e_send, recv_sem=e_recv,
            device_id=(section, peer_of(k)), device_id_type=MESH).start()

    @pl.loop(0, blocks)
    def _(o):
        found = jnp.int32(0)
        for b in range(blocks):
            found = jnp.where(owners[b] == o, jnp.int32(b), found)
        inverse[o] = found

    others = pl.ds(0, groups - 1)
    energy_wait = pltpu.make_async_remote_copy(
        src_ref=parts.at[others], dst_ref=parts.at[others], send_sem=e_send, recv_sem=e_recv,
        device_id=(section, peer_of(1)), device_id_type=MESH)
    energy_wait.wait_recv()
    total = parts[0]
    for g in range(1, groups):
        total = total + parts[g]
    row = jnp.sum(total, axis=1, keepdims=True)
    energy = row
    for i in range(1, per_tile):
        energy = energy + jnp.concatenate([row[i * layers:], row[:i * layers]], axis=0)
    scale = 1.0 / jnp.sqrt(energy * (1.0 / (tokens * groups * features)) + 1.0)
    scale = jnp.concatenate([scale] * (rows // SUBLANES), axis=0)

    for k in range(chunks):
        for d in range(groups):
            for j in range(per_dev):
                lane = d * width + k * LANES
                s1[k, d * per_dev + j] = (
                    centered[j * rows:(j + 1) * rows, lane:lane + LANES] * scale).astype(jnp.bfloat16)
        mine = pl.ds(group * per_dev, per_dev)
        for p in range(1, groups):
            d = peer_of(p)
            pltpu.make_async_remote_copy(
                src_ref=s1.at[k, pl.ds(d * per_dev, per_dev)], dst_ref=r1[k].at[mine],
                send_sem=send1.at[k], recv_sem=recv1.at[k],
                device_id=(section, d), device_id_type=MESH).start()
        r1[k][mine] = s1[k, mine]

    for k in range(chunks):
        span = pl.ds(0, (groups - 1) * per_dev)
        pltpu.make_async_remote_copy(
            src_ref=r1[k].at[span], dst_ref=r1[k].at[span], send_sem=send1.at[k], recv_sem=recv1.at[k],
            device_id=(section, peer_of(1)), device_id_type=MESH).wait_recv()
        for o in range(devices):
            s2[k, o] = r1[k][inverse[o]]
        for p in range(1, devices):
            o = lax.rem(me + p, devices)
            pltpu.make_async_remote_copy(
                src_ref=s2.at[k, o], dst_ref=r2.at[k, me],
                send_sem=send2.at[k], recv_sem=recv2.at[k],
                device_id=(o // groups, lax.rem(o, groups)), device_id_type=MESH).start()
        r2[k, me] = s2[k, me]

    for k in range(chunks):
        span = pl.ds(0, devices - 1)
        pltpu.make_async_remote_copy(
            src_ref=r2.at[k, span], dst_ref=r2.at[k, span], send_sem=send2.at[k], recv_sem=recv2.at[k],
            device_id=(section, peer_of(1)), device_id_type=MESH).wait_recv()
        for d in range(groups):
            got = [r2[k, s * groups + d].astype(jnp.float32) for s in range(sections)]
            lane = d * width + k * LANES
            for i in range(block_len):
                out_ref[i, :, lane:lane + LANES] = jnp.concatenate(
                    [v[i * layers:(i + 1) * layers] for v in got], axis=0).astype(jnp.bfloat16)

    energy_wait.wait_send()
    for k in range(chunks):
        span = pl.ds(0, (groups - 1) * per_dev)
        pltpu.make_async_remote_copy(
            src_ref=s1.at[k, span], dst_ref=r1[k].at[span], send_sem=send1.at[k], recv_sem=recv1.at[k],
            device_id=(section, peer_of(1)), device_id_type=MESH).wait_send()
        span = pl.ds(0, devices - 1)
        pltpu.make_async_remote_copy(
            src_ref=s2.at[k, span], dst_ref=r2.at[k, span], send_sem=send2.at[k], recv_sem=recv2.at[k],
            device_id=(section, peer_of(1)), device_id_type=MESH).wait_send()


def solution(mesh):
    sections, groups = mesh.shape["section"], mesh.shape["dp"]

    def on_device(residuals, owners):
        layers, tokens, features = residuals.shape
        blocks = owners.shape[0]
        block_len = tokens * groups // blocks
        rows = block_len * layers
        chunks = features // groups // LANES
        tiles = (chunks, blocks, rows, LANES)
        dma = pltpu.SemaphoreType.DMA
        return pl.pallas_call(
            functools.partial(harvest_kernel, sections, groups),
            out_shape=jax.ShapeDtypeStruct((block_len, layers * sections, features), jnp.bfloat16),
            in_specs=[pl.BlockSpec(memory_space=pl.ANY), pl.BlockSpec(memory_space=pltpu.SMEM)],
            out_specs=pl.BlockSpec(memory_space=pltpu.VMEM),
            scratch_shapes=[
                pltpu.SMEM((blocks,), jnp.int32),
                pltpu.VMEM((layers, tokens, features), jnp.float32),
                pltpu.VMEM((layers * tokens, features), jnp.float32),
                pltpu.VMEM((SUBLANES, LANES), jnp.float32),
                pltpu.VMEM((groups, SUBLANES, LANES), jnp.float32),
                pltpu.VMEM(tiles, jnp.bfloat16),
                pltpu.VMEM(tiles, jnp.bfloat16),
                pltpu.VMEM(tiles, jnp.bfloat16),
                dma, dma, dma,
                dma((chunks,)), dma((chunks,)), dma((chunks,)), dma((chunks,)),
                *[pltpu.VMEM(tiles[1:], jnp.bfloat16) for _ in range(chunks)],
            ],
            compiler_params=pltpu.CompilerParams(collective_id=0, has_side_effects=True),
            name="harvest",
        )(residuals, owners)

    in_specs = (P("section", "dp", None), P())
    out_specs = P(("section", "dp"), None, None)
    return jax.shard_map(on_device, mesh=mesh, in_specs=in_specs, out_specs=out_specs, check_vma=False)
```

```python
import functools

import jax
import jax.numpy as jnp
from jax import lax
from jax.experimental import pallas as pl
from jax.experimental.pallas import tpu as pltpu
from jax.sharding import PartitionSpec as P

MESH = pl.DeviceIdType.MESH
LANES = 128
SUBLANES = 8


def harvest_kernel(sections, groups, early, x_hbm, owners_hbm, out_ref, owners, inverse, xv, centered, part, parts,
                   s1, s2, r2, x_sem, o_sem, e_send, e_recv, send1, recv1, send2, recv2, *r1):
    layers, tokens, features = x_hbm.shape
    chunks, blocks, rows, _ = s1.shape
    width = features // groups
    block_len = rows // layers
    per_dev = tokens // block_len
    devices = sections * groups
    section, group = lax.axis_index("section"), lax.axis_index("dp")
    me = section * groups + group

    load = pltpu.make_async_copy(x_hbm, xv, x_sem)
    load.start()
    barrier = pltpu.get_barrier_semaphore()

    def peer_of(k):
        return lax.rem(group + k, groups)

    for k in range(1, groups):
        pl.semaphore_signal(barrier, inc=1, device_id=(section, peer_of(k)), device_id_type=MESH)
    for k in range(1, sections):
        pl.semaphore_signal(barrier, inc=1, device_id=(lax.rem(section + k, sections), group), device_id_type=MESH)

    load_owners = pltpu.make_async_copy(owners_hbm, owners, o_sem)
    load_owners.start()
    load.wait()
    per_tile = SUBLANES // layers
    acc = jnp.zeros((SUBLANES, LANES), jnp.float32)
    for g in range(tokens // per_tile):
        x8 = jnp.concatenate([xv[:, g * per_tile + i, :] for i in range(per_tile)], axis=0)
        c = x8 - jnp.sum(x8, axis=1, keepdims=True) * (1.0 / features)
        j, r = divmod(g * SUBLANES, rows)
        sq = c * c
        for f in range(features // LANES):
            centered[f, j, r:r + SUBLANES] = c[:, f * LANES:(f + 1) * LANES]
            acc = acc + sq[:, f * LANES:(f + 1) * LANES]
    part[...] = acc
    parts[group] = acc

    pl.semaphore_wait(barrier, groups + sections - 2)
    for k in range(1, groups):
        pltpu.make_async_remote_copy(
            src_ref=part, dst_ref=parts.at[group], send_sem=e_send, recv_sem=e_recv,
            device_id=(section, peer_of(k)), device_id_type=MESH).start()

    mine = pl.ds(group * per_dev, per_dev)

    def spread(k, source):
        for p in range(1, groups):
            d = peer_of(p)
            pltpu.make_async_remote_copy(
                src_ref=source(d), dst_ref=r1[k].at[mine], send_sem=send1.at[k], recv_sem=recv1.at[k],
                device_id=(section, d), device_id_type=MESH).start()
        r1[k][mine] = source(group)[...]

    for k in range(early):
        spread(k, lambda d: centered.at[d * chunks + k])

    load_owners.wait()

    @pl.loop(0, blocks)
    def _(o):
        found = jnp.int32(0)
        for b in range(blocks):
            found = jnp.where(owners[b] == o, jnp.int32(b), found)
        inverse[o] = found

    others = pl.ds(0, groups - 1)
    energy_wait = pltpu.make_async_remote_copy(
        src_ref=parts.at[others], dst_ref=parts.at[others], send_sem=e_send, recv_sem=e_recv,
        device_id=(section, peer_of(1)), device_id_type=MESH)
    energy_wait.wait_recv()
    total = parts[0]
    for g in range(1, groups):
        total = total + parts[g]
    row = jnp.sum(total, axis=1, keepdims=True)
    energy = row
    for i in range(1, per_tile):
        energy = energy + jnp.concatenate([row[i * layers:], row[:i * layers]], axis=0)
    scale = 1.0 / jnp.sqrt(energy * (1.0 / (tokens * groups * features)) + 1.0)
    scale = jnp.concatenate([scale] * (rows // SUBLANES), axis=0)

    for k in range(early, chunks):
        for d in range(groups):
            for j in range(per_dev):
                s1[k, d * per_dev + j] = (centered[d * chunks + k, j] * scale).astype(jnp.bfloat16)
        spread(k, lambda d: s1.at[k, pl.ds(d * per_dev, per_dev)])

    for k in range(chunks):
        span = pl.ds(0, (groups - 1) * per_dev)
        pltpu.make_async_remote_copy(
            src_ref=r1[k].at[span], dst_ref=r1[k].at[span], send_sem=send1.at[k], recv_sem=recv1.at[k],
            device_id=(section, peer_of(1)), device_id_type=MESH).wait_recv()
        for o in range(devices):
            block = r1[k][inverse[o]]
            s2[k, o] = (block * scale).astype(jnp.bfloat16) if k < early else block
        for p in range(1, devices):
            o = lax.rem(me + p, devices)
            pltpu.make_async_remote_copy(
                src_ref=s2.at[k, o], dst_ref=r2.at[k, me],
                send_sem=send2.at[k], recv_sem=recv2.at[k],
                device_id=(o // groups, lax.rem(o, groups)), device_id_type=MESH).start()
        r2[k, me] = s2[k, me]

    for k in range(chunks):
        span = pl.ds(0, devices - 1)
        pltpu.make_async_remote_copy(
            src_ref=r2.at[k, span], dst_ref=r2.at[k, span], send_sem=send2.at[k], recv_sem=recv2.at[k],
            device_id=(section, peer_of(1)), device_id_type=MESH).wait_recv()
        for d in range(groups):
            got = [r2[k, s * groups + d].astype(jnp.float32) for s in range(sections)]
            lane = d * width + k * LANES
            for i in range(block_len):
                out_ref[i, :, lane:lane + LANES] = jnp.concatenate(
                    [v[i * layers:(i + 1) * layers] for v in got], axis=0).astype(jnp.bfloat16)

    energy_wait.wait_send()
    for k in range(chunks):
        span = pl.ds(0, (groups - 1) * per_dev)
        pltpu.make_async_remote_copy(
            src_ref=r1[k].at[span], dst_ref=r1[k].at[span], send_sem=send1.at[k], recv_sem=recv1.at[k],
            device_id=(section, peer_of(1)), device_id_type=MESH).wait_send()
        span = pl.ds(0, devices - 1)
        pltpu.make_async_remote_copy(
            src_ref=s2.at[k, span], dst_ref=r2.at[k, span], send_sem=send2.at[k], recv_sem=recv2.at[k],
            device_id=(section, peer_of(1)), device_id_type=MESH).wait_send()


def solution(mesh):
    sections, groups = mesh.shape["section"], mesh.shape["dp"]

    def on_device(residuals, owners):
        layers, tokens, features = residuals.shape
        blocks = owners.shape[0]
        block_len = tokens * groups // blocks
        rows = block_len * layers
        chunks = features // groups // LANES
        early = chunks // 2
        tiles = (chunks, blocks, rows, LANES)
        dma = pltpu.SemaphoreType.DMA
        return pl.pallas_call(
            functools.partial(harvest_kernel, sections, groups, early),
            out_shape=jax.ShapeDtypeStruct((block_len, layers * sections, features), jnp.bfloat16),
            in_specs=[pl.BlockSpec(memory_space=pl.ANY), pl.BlockSpec(memory_space=pl.ANY)],
            out_specs=pl.BlockSpec(memory_space=pltpu.VMEM),
            scratch_shapes=[
                pltpu.SMEM((blocks,), jnp.int32),
                pltpu.SMEM((blocks,), jnp.int32),
                pltpu.VMEM((layers, tokens, features), jnp.float32),
                pltpu.VMEM((features // LANES, blocks // groups, rows, LANES), jnp.float32),
                pltpu.VMEM((SUBLANES, LANES), jnp.float32),
                pltpu.VMEM((groups, SUBLANES, LANES), jnp.float32),
                pltpu.VMEM(tiles, jnp.bfloat16),
                pltpu.VMEM(tiles, jnp.bfloat16),
                pltpu.VMEM(tiles, jnp.bfloat16),
                dma, dma, dma, dma,
                dma((chunks,)), dma((chunks,)), dma((chunks,)), dma((chunks,)),
                *[pltpu.VMEM(tiles[1:], jnp.float32 if k < early else jnp.bfloat16) for k in range(chunks)],
            ],
            compiler_params=pltpu.CompilerParams(collective_id=0, has_side_effects=True),
            name="harvest",
        )(residuals, owners)

    in_specs = (P("section", "dp", None), P())
    out_specs = P(("section", "dp"), None, None)
    return jax.shard_map(on_device, mesh=mesh, in_specs=in_specs, out_specs=out_specs, check_vma=False)
```

```python
import functools

import jax
import jax.numpy as jnp
from jax import lax
from jax.experimental import pallas as pl
from jax.experimental.pallas import tpu as pltpu
from jax.sharding import PartitionSpec as P

MESH = pl.DeviceIdType.MESH
LANES = 128
SUBLANES = 8


def harvest_kernel(sections, groups, early, x_hbm, owners_hbm, r2, owners, inverse, xv, centered, part, parts,
                   s1, s2, x_sem, o_sem, e_send, e_recv, send1, recv1, send2, recv2, *r1):
    layers, tokens, features = x_hbm.shape
    chunks, blocks, rows, _ = s1.shape
    width = features // groups
    block_len = rows // layers
    per_dev = tokens // block_len
    devices = sections * groups
    section, group = lax.axis_index("section"), lax.axis_index("dp")
    me = section * groups + group

    load = pltpu.make_async_copy(x_hbm, xv, x_sem)
    load.start()
    barrier = pltpu.get_barrier_semaphore()

    def peer_of(k):
        return lax.rem(group + k, groups)

    for k in range(1, groups):
        pl.semaphore_signal(barrier, inc=1, device_id=(section, peer_of(k)), device_id_type=MESH)
    for k in range(1, sections):
        pl.semaphore_signal(barrier, inc=1, device_id=(lax.rem(section + k, sections), group), device_id_type=MESH)

    load_owners = pltpu.make_async_copy(owners_hbm, owners, o_sem)
    load_owners.start()
    load.wait()
    per_tile = SUBLANES // layers
    acc = jnp.zeros((SUBLANES, LANES), jnp.float32)
    for g in range(tokens // per_tile):
        x8 = jnp.concatenate([xv[:, g * per_tile + i, :] for i in range(per_tile)], axis=0)
        c = x8 - jnp.sum(x8, axis=1, keepdims=True) * (1.0 / features)
        j, r = divmod(g * SUBLANES, rows)
        sq = c * c
        for f in range(features // LANES):
            centered[f, j, r:r + SUBLANES] = c[:, f * LANES:(f + 1) * LANES]
            acc = acc + sq[:, f * LANES:(f + 1) * LANES]
    part[...] = acc
    parts[group] = acc

    pl.semaphore_wait(barrier, groups + sections - 2)
    for k in range(1, groups):
        pltpu.make_async_remote_copy(
            src_ref=part, dst_ref=parts.at[group], send_sem=e_send, recv_sem=e_recv,
            device_id=(section, peer_of(k)), device_id_type=MESH).start()

    mine = pl.ds(group * per_dev, per_dev)

    def spread(k, source):
        for p in range(1, groups):
            d = peer_of(p)
            pltpu.make_async_remote_copy(
                src_ref=source(d), dst_ref=r1[k].at[mine], send_sem=send1.at[k], recv_sem=recv1.at[k],
                device_id=(section, d), device_id_type=MESH).start()
        r1[k][mine] = source(group)[...]

    for k in range(early):
        spread(k, lambda d: centered.at[d * chunks + k])

    load_owners.wait()

    @pl.loop(0, blocks)
    def _(o):
        found = jnp.int32(0)
        for b in range(blocks):
            found = jnp.where(owners[b] == o, jnp.int32(b), found)
        inverse[o] = found

    others = pl.ds(0, groups - 1)
    energy_wait = pltpu.make_async_remote_copy(
        src_ref=parts.at[others], dst_ref=parts.at[others], send_sem=e_send, recv_sem=e_recv,
        device_id=(section, peer_of(1)), device_id_type=MESH)
    energy_wait.wait_recv()
    total = parts[0]
    for g in range(1, groups):
        total = total + parts[g]
    row = jnp.sum(total, axis=1, keepdims=True)
    energy = row
    for i in range(1, per_tile):
        energy = energy + jnp.concatenate([row[i * layers:], row[:i * layers]], axis=0)
    scale = 1.0 / jnp.sqrt(energy * (1.0 / (tokens * groups * features)) + 1.0)
    scale = jnp.concatenate([scale] * (rows // SUBLANES), axis=0)

    for k in range(early, chunks):
        for d in range(groups):
            for j in range(per_dev):
                s1[k, d * per_dev + j] = (centered[d * chunks + k, j] * scale).astype(jnp.bfloat16)
        spread(k, lambda d: s1.at[k, pl.ds(d * per_dev, per_dev)])

    for k in range(chunks):
        span = pl.ds(0, (groups - 1) * per_dev)
        pltpu.make_async_remote_copy(
            src_ref=r1[k].at[span], dst_ref=r1[k].at[span], send_sem=send1.at[k], recv_sem=recv1.at[k],
            device_id=(section, peer_of(1)), device_id_type=MESH).wait_recv()
        for o in range(devices):
            block = r1[k][inverse[o]]
            s2[k, o] = (block * scale).astype(jnp.bfloat16) if k < early else block
        for p in range(1, devices):
            o = lax.rem(me + p, devices)
            pltpu.make_async_remote_copy(
                src_ref=s2.at[k, o], dst_ref=r2.at[k, me],
                send_sem=send2.at[k], recv_sem=recv2.at[k],
                device_id=(o // groups, lax.rem(o, groups)), device_id_type=MESH).start()
        r2[k, me] = s2[k, me]

    for k in range(chunks):
        span = pl.ds(0, devices - 1)
        pltpu.make_async_remote_copy(
            src_ref=r2.at[k, span], dst_ref=r2.at[k, span], send_sem=send2.at[k], recv_sem=recv2.at[k],
            device_id=(section, peer_of(1)), device_id_type=MESH).wait_recv()
    energy_wait.wait_send()
    for k in range(chunks):
        span = pl.ds(0, (groups - 1) * per_dev)
        pltpu.make_async_remote_copy(
            src_ref=r1[k].at[span], dst_ref=r1[k].at[span], send_sem=send1.at[k], recv_sem=recv1.at[k],
            device_id=(section, peer_of(1)), device_id_type=MESH).wait_send()
        span = pl.ds(0, devices - 1)
        pltpu.make_async_remote_copy(
            src_ref=s2.at[k, span], dst_ref=r2.at[k, span], send_sem=send2.at[k], recv_sem=recv2.at[k],
            device_id=(section, peer_of(1)), device_id_type=MESH).wait_send()


def assemble_kernel(sections, groups, r2, out_ref):
    block_len, all_layers, features = out_ref.shape
    layers = all_layers // sections
    chunks = r2.shape[0]
    width = features // groups
    for k in range(chunks):
        for d in range(groups):
            got = [r2[k, s * groups + d].astype(jnp.float32) for s in range(sections)]
            lane = d * width + k * LANES
            for i in range(block_len):
                out_ref[i, :, lane:lane + LANES] = jnp.concatenate(
                    [v[i * layers:(i + 1) * layers] for v in got], axis=0).astype(jnp.bfloat16)


def solution(mesh):
    sections, groups = mesh.shape["section"], mesh.shape["dp"]

    def on_device(residuals, owners):
        layers, tokens, features = residuals.shape
        blocks = owners.shape[0]
        block_len = tokens * groups // blocks
        rows = block_len * layers
        chunks = features // groups // LANES
        early = 0
        tiles = (chunks, blocks, rows, LANES)
        dma = pltpu.SemaphoreType.DMA
        received = pl.pallas_call(
            functools.partial(harvest_kernel, sections, groups, early),
            out_shape=pltpu.VMEM(tiles, jnp.bfloat16),
            in_specs=[pl.BlockSpec(memory_space=pl.ANY), pl.BlockSpec(memory_space=pl.ANY)],
            out_specs=pl.BlockSpec(memory_space=pltpu.VMEM),
            scratch_shapes=[
                pltpu.SMEM((blocks,), jnp.int32),
                pltpu.SMEM((blocks,), jnp.int32),
                pltpu.VMEM((layers, tokens, features), jnp.float32),
                pltpu.VMEM((features // LANES, blocks // groups, rows, LANES), jnp.float32),
                pltpu.VMEM((SUBLANES, LANES), jnp.float32),
                pltpu.VMEM((groups, SUBLANES, LANES), jnp.float32),
                pltpu.VMEM(tiles, jnp.bfloat16),
                pltpu.VMEM(tiles, jnp.bfloat16),
                dma, dma, dma, dma,
                dma((chunks,)), dma((chunks,)), dma((chunks,)), dma((chunks,)),
                *[pltpu.VMEM(tiles[1:], jnp.float32 if k < early else jnp.bfloat16) for k in range(chunks)],
            ],
            compiler_params=pltpu.CompilerParams(collective_id=0, has_side_effects=True),
            name="harvest",
        )(residuals, owners)
        return pl.pallas_call(
            functools.partial(assemble_kernel, sections, groups),
            out_shape=jax.ShapeDtypeStruct((block_len, layers * sections, features), jnp.bfloat16),
            in_specs=[pl.BlockSpec(memory_space=pltpu.VMEM)],
            out_specs=pl.BlockSpec(memory_space=pltpu.VMEM),
            name="assemble",
        )(pltpu.with_memory_space_constraint(received, pltpu.VMEM))

    in_specs = (P("section", "dp", None), P())
    out_specs = P(("section", "dp"), None, None)
    return jax.shard_map(on_device, mesh=mesh, in_specs=in_specs, out_specs=out_specs, check_vma=False)
```

```python
import functools

import jax
import jax.numpy as jnp
from jax import lax
from jax.experimental import pallas as pl
from jax.experimental.pallas import tpu as pltpu
from jax.sharding import PartitionSpec as P

MESH = pl.DeviceIdType.MESH
LANES = 128
SUBLANES = 8


def harvest_kernel(sections, groups, early, x_hbm, owners_hbm, r2, owners, inverse, xv, centered, part, parts,
                   s1, s2, x_sem, o_sem, e_send, e_recv, send1, recv1, send2, recv2, *r1):
    layers, tokens, features = x_hbm.shape
    chunks, blocks, rows, _ = s1.shape
    width = features // groups
    block_len = rows // layers
    per_dev = tokens // block_len
    devices = sections * groups
    section, group = lax.axis_index("section"), lax.axis_index("dp")
    me = section * groups + group

    load = pltpu.make_async_copy(x_hbm, xv, x_sem)
    load.start()
    barrier = pltpu.get_barrier_semaphore()

    def peer_of(k):
        return lax.rem(group + k, groups)

    for k in range(1, groups):
        pl.semaphore_signal(barrier, inc=1, device_id=(section, peer_of(k)), device_id_type=MESH)
    for k in range(1, sections):
        pl.semaphore_signal(barrier, inc=1, device_id=(lax.rem(section + k, sections), group), device_id_type=MESH)

    load_owners = pltpu.make_async_copy(owners_hbm, owners, o_sem)
    load_owners.start()
    load.wait()
    per_tile = SUBLANES // layers
    acc = jnp.zeros((SUBLANES, LANES), jnp.float32)
    for g in range(tokens // per_tile):
        x8 = jnp.concatenate([xv[:, g * per_tile + i, :] for i in range(per_tile)], axis=0)
        c = x8 - jnp.sum(x8, axis=1, keepdims=True) * (1.0 / features)
        j, r = divmod(g * SUBLANES, rows)
        sq = c * c
        for f in range(features // LANES):
            centered[f, j, r:r + SUBLANES] = c[:, f * LANES:(f + 1) * LANES]
            acc = acc + sq[:, f * LANES:(f + 1) * LANES]
    lane = lax.broadcasted_iota(jnp.int32, (SUBLANES, LANES), 1)
    row = lax.broadcasted_iota(jnp.int32, (SUBLANES, LANES), 0)
    own_lanes = lane // (LANES // layers) == row % layers
    fold = LANES // 2
    while fold >= LANES // layers:
        acc = acc + pltpu.roll(acc, fold, 1)
        fold //= 2
    acc = jnp.sum(jnp.where(own_lanes, acc, 0.0), axis=0, keepdims=True)
    part[...] = acc
    parts[group] = acc

    pl.semaphore_wait(barrier, groups + sections - 2)
    order = sorted(range(1, groups), key=lambda p: min(p, groups - p))
    for k in order:
        pltpu.make_async_remote_copy(
            src_ref=part, dst_ref=parts.at[group], send_sem=e_send, recv_sem=e_recv,
            device_id=(section, peer_of(k)), device_id_type=MESH).start()

    mine = pl.ds(group * per_dev, per_dev)

    def spread(k, source):
        for p in order:
            d = peer_of(p)
            pltpu.make_async_remote_copy(
                src_ref=source(d), dst_ref=r1[k].at[mine], send_sem=send1.at[k], recv_sem=recv1.at[k],
                device_id=(section, d), device_id_type=MESH).start()
        r1[k][mine] = source(group)[...]

    for k in range(early):
        spread(k, lambda d: centered.at[d * chunks + k])

    load_owners.wait()

    @pl.loop(0, blocks)
    def _(o):
        found = jnp.int32(0)
        for b in range(blocks):
            found = jnp.where(owners[b] == o, jnp.int32(b), found)
        inverse[o] = found

    others = pl.ds(0, groups - 1)
    energy_wait = pltpu.make_async_remote_copy(
        src_ref=parts.at[others], dst_ref=parts.at[others], send_sem=e_send, recv_sem=e_recv,
        device_id=(section, peer_of(1)), device_id_type=MESH)
    energy_wait.wait_recv()
    total = parts[0]
    for g in range(1, groups):
        total = total + parts[g]
    energy = jnp.sum(jnp.where(own_lanes, total, 0.0), axis=1, keepdims=True)
    scale = 1.0 / jnp.sqrt(energy * (1.0 / (tokens * groups * features)) + 1.0)
    scale = jnp.concatenate([scale] * (rows // SUBLANES), axis=0)

    for k in range(early, chunks):
        for d in range(groups):
            for j in range(per_dev):
                s1[k, d * per_dev + j] = (centered[d * chunks + k, j] * scale).astype(jnp.bfloat16)
        spread(k, lambda d: s1.at[k, pl.ds(d * per_dev, per_dev)])

    for k in range(chunks):
        span = pl.ds(0, (groups - 1) * per_dev)
        pltpu.make_async_remote_copy(
            src_ref=r1[k].at[span], dst_ref=r1[k].at[span], send_sem=send1.at[k], recv_sem=recv1.at[k],
            device_id=(section, peer_of(1)), device_id_type=MESH).wait_recv()
        for o in range(devices):
            block = r1[k][inverse[o]]
            s2[k, o] = (block * scale).astype(jnp.bfloat16) if k < early else block
        for p, q in [(p, q) for p in order + [0] for q in range(sections) if p or q]:
            sec, d = lax.rem(section + q, sections), peer_of(p)
            o = sec * groups + d
            pltpu.make_async_remote_copy(
                src_ref=s2.at[k, o], dst_ref=r2.at[k, me],
                send_sem=send2.at[k], recv_sem=recv2.at[k],
                device_id=(sec, d), device_id_type=MESH).start()
        r2[k, me] = s2[k, me]

    for k in range(chunks):
        span = pl.ds(0, devices - 1)
        pltpu.make_async_remote_copy(
            src_ref=r2.at[k, span], dst_ref=r2.at[k, span], send_sem=send2.at[k], recv_sem=recv2.at[k],
            device_id=(section, peer_of(1)), device_id_type=MESH).wait_recv()
    energy_wait.wait_send()
    for k in range(chunks):
        span = pl.ds(0, (groups - 1) * per_dev)
        pltpu.make_async_remote_copy(
            src_ref=r1[k].at[span], dst_ref=r1[k].at[span], send_sem=send1.at[k], recv_sem=recv1.at[k],
            device_id=(section, peer_of(1)), device_id_type=MESH).wait_send()
        span = pl.ds(0, devices - 1)
        pltpu.make_async_remote_copy(
            src_ref=s2.at[k, span], dst_ref=r2.at[k, span], send_sem=send2.at[k], recv_sem=recv2.at[k],
            device_id=(section, peer_of(1)), device_id_type=MESH).wait_send()


def assemble_kernel(sections, groups, r2, out_ref):
    block_len, all_layers, features = out_ref.shape
    layers = all_layers // sections
    chunks = r2.shape[0]
    width = features // groups
    for k in range(chunks):
        for d in range(groups):
            got = [r2[k, s * groups + d].astype(jnp.float32) for s in range(sections)]
            lane = d * width + k * LANES
            for i in range(block_len):
                out_ref[i, :, lane:lane + LANES] = jnp.concatenate(
                    [v[i * layers:(i + 1) * layers] for v in got], axis=0).astype(jnp.bfloat16)


def solution(mesh):
    sections, groups = mesh.shape["section"], mesh.shape["dp"]

    def on_device(residuals, owners):
        layers, tokens, features = residuals.shape
        blocks = owners.shape[0]
        block_len = tokens * groups // blocks
        rows = block_len * layers
        chunks = features // groups // LANES
        early = 0
        tiles = (chunks, blocks, rows, LANES)
        dma = pltpu.SemaphoreType.DMA
        received = pl.pallas_call(
            functools.partial(harvest_kernel, sections, groups, early),
            out_shape=pltpu.VMEM(tiles, jnp.bfloat16),
            in_specs=[pl.BlockSpec(memory_space=pl.ANY), pl.BlockSpec(memory_space=pl.ANY)],
            out_specs=pl.BlockSpec(memory_space=pltpu.VMEM),
            scratch_shapes=[
                pltpu.SMEM((blocks,), jnp.int32),
                pltpu.SMEM((blocks,), jnp.int32),
                pltpu.VMEM((layers, tokens, features), jnp.float32),
                pltpu.VMEM((features // LANES, blocks // groups, rows, LANES), jnp.float32),
                pltpu.VMEM((1, LANES), jnp.float32),
                pltpu.VMEM((groups, 1, LANES), jnp.float32),
                pltpu.VMEM(tiles, jnp.bfloat16),
                pltpu.VMEM(tiles, jnp.bfloat16),
                dma, dma, dma, dma,
                dma((chunks,)), dma((chunks,)), dma((chunks,)), dma((chunks,)),
                *[pltpu.VMEM(tiles[1:], jnp.float32 if k < early else jnp.bfloat16) for k in range(chunks)],
            ],
            compiler_params=pltpu.CompilerParams(collective_id=0, has_side_effects=True),
            name="harvest",
        )(residuals, owners)
        return pl.pallas_call(
            functools.partial(assemble_kernel, sections, groups),
            out_shape=jax.ShapeDtypeStruct((block_len, layers * sections, features), jnp.bfloat16),
            in_specs=[pl.BlockSpec(memory_space=pltpu.VMEM)],
            out_specs=pl.BlockSpec(memory_space=pltpu.VMEM),
            name="assemble",
        )(pltpu.with_memory_space_constraint(received, pltpu.VMEM))

    in_specs = (P("section", "dp", None), P())
    out_specs = P(("section", "dp"), None, None)
    return jax.shard_map(on_device, mesh=mesh, in_specs=in_specs, out_specs=out_specs, check_vma=False)
```

```python
import functools

import jax
import jax.numpy as jnp
from jax import lax
from jax.experimental import pallas as pl
from jax.experimental.pallas import tpu as pltpu
from jax.sharding import PartitionSpec as P

MESH = pl.DeviceIdType.MESH
LANES = 128
SUBLANES = 8


def harvest_kernel(sections, groups, early, x_hbm, owners_hbm, out_ref, owners, inverse, xv, centered, part, parts,
                   late, s1, s2, r2, x_sem, o_sem, e_send, e_recv, send1, recv1, send2, recv2, *r1):
    half = s1.shape[2] // 2
    layers, tokens, features = x_hbm.shape
    chunks, blocks, rows, _ = s1.shape
    width = features // groups
    block_len = rows // layers
    per_dev = tokens // block_len
    devices = sections * groups
    section, group = lax.axis_index("section"), lax.axis_index("dp")
    me = section * groups + group

    load = pltpu.make_async_copy(x_hbm, xv, x_sem)
    load.start()
    barrier = pltpu.get_barrier_semaphore()

    def peer_of(k):
        return lax.rem(group + k, groups)

    for k in range(1, groups):
        pl.semaphore_signal(barrier, inc=1, device_id=(section, peer_of(k)), device_id_type=MESH)
    for k in range(1, sections):
        pl.semaphore_signal(barrier, inc=1, device_id=(lax.rem(section + k, sections), group), device_id_type=MESH)

    load_owners = pltpu.make_async_copy(owners_hbm, owners, o_sem)
    load_owners.start()
    load.wait()
    per_tile = SUBLANES // layers
    acc = jnp.zeros((SUBLANES, LANES), jnp.float32)
    for g in range(tokens // per_tile):
        x8 = jnp.concatenate([xv[:, g * per_tile + i, :] for i in range(per_tile)], axis=0)
        c = x8 - jnp.sum(x8, axis=1, keepdims=True) * (1.0 / features)
        j, r = divmod(g * SUBLANES, rows)
        sq = c * c
        for f in range(features // LANES):
            centered[f, j, r:r + SUBLANES] = c[:, f * LANES:(f + 1) * LANES]
            acc = acc + sq[:, f * LANES:(f + 1) * LANES]
    lane = lax.broadcasted_iota(jnp.int32, (SUBLANES, LANES), 1)
    row = lax.broadcasted_iota(jnp.int32, (SUBLANES, LANES), 0)
    own_lanes = lane // (LANES // layers) == row % layers
    fold = LANES // 2
    while fold >= LANES // layers:
        acc = acc + pltpu.roll(acc, fold, 1)
        fold //= 2
    acc = jnp.sum(jnp.where(own_lanes, acc, 0.0), axis=0, keepdims=True)
    part[...] = acc
    parts[group] = acc

    pl.semaphore_wait(barrier, groups + sections - 2)
    order = sorted(range(1, groups), key=lambda p: min(p, groups - p))
    early_order = sorted(range(1, groups), key=lambda p: min(p, groups - p))
    first_order = sorted(range(1, groups), key=lambda p: min(p, groups - p))
    second_order = list(range(1, groups))
    for k in order:
        pltpu.make_async_remote_copy(
            src_ref=part, dst_ref=parts.at[group], send_sem=e_send, recv_sem=e_recv,
            device_id=(section, peer_of(k)), device_id_type=MESH).start()

    mine = pl.ds(group * per_dev, per_dev)
    units = len(r1)

    def spread(u, source):
        for p in (early_order if u == chunks else first_order):
            d = peer_of(p)
            pltpu.make_async_remote_copy(
                src_ref=source(d), dst_ref=r1[u].at[mine], send_sem=send1.at[u], recv_sem=recv1.at[u],
                device_id=(section, d), device_id_type=MESH).start()
        r1[u][mine] = source(group)[...]

    if early:
        spread(chunks, lambda d: centered.at[d * chunks, :, pl.ds(0, half)])

    load_owners.wait()

    @pl.loop(0, blocks)
    def _(o):
        found = jnp.int32(0)
        for b in range(blocks):
            found = jnp.where(owners[b] == o, jnp.int32(b), found)
        inverse[o] = found

    others = pl.ds(0, groups - 1)
    energy_wait = pltpu.make_async_remote_copy(
        src_ref=parts.at[others], dst_ref=parts.at[others], send_sem=e_send, recv_sem=e_recv,
        device_id=(section, peer_of(1)), device_id_type=MESH)
    energy_wait.wait_recv()
    total = parts[0]
    for g in range(1, groups):
        total = total + parts[g]
    energy = jnp.sum(jnp.where(own_lanes, total, 0.0), axis=1, keepdims=True)
    scale = 1.0 / jnp.sqrt(energy * (1.0 / (tokens * groups * features)) + 1.0)
    scale = jnp.concatenate([scale] * (rows // SUBLANES), axis=0)

    for k in range(chunks):
        top = half if early and k == 0 else 0
        for d in range(groups):
            for j in range(per_dev):
                b = d * per_dev + j
                if top:
                    late[b] = (centered[d * chunks, j, top:] * scale[top:]).astype(jnp.bfloat16)
                else:
                    s1[k, b] = (centered[d * chunks + k, j] * scale).astype(jnp.bfloat16)
        if top:
            spread(k, lambda d: late.at[pl.ds(d * per_dev, per_dev)])
        else:
            spread(k, lambda d: s1.at[k, pl.ds(d * per_dev, per_dev)])

    def arrived(u):
        span = pl.ds(0, (groups - 1) * per_dev)
        return pltpu.make_async_remote_copy(
            src_ref=r1[u].at[span], dst_ref=r1[u].at[span], send_sem=send1.at[u], recv_sem=recv1.at[u],
            device_id=(section, peer_of(1)), device_id_type=MESH)

    if early:
        arrived(chunks).wait_recv()
    for k in range(chunks):
        arrived(k).wait_recv()
        for o in range(devices):
            b = inverse[o]
            if early and k == 0:
                first = r1[chunks][b] * scale[:half]
                s2[k, o] = jnp.concatenate([first, r1[k][b].astype(jnp.float32)], axis=0).astype(jnp.bfloat16)
            else:
                s2[k, o] = r1[k][b]
        for p, q in [(p, q) for p in second_order + [0] for q in range(sections) if p or q]:
            sec, d = lax.rem(section + q, sections), peer_of(p)
            o = sec * groups + d
            pltpu.make_async_remote_copy(
                src_ref=s2.at[k, o], dst_ref=r2.at[k, me],
                send_sem=send2.at[k], recv_sem=recv2.at[k],
                device_id=(sec, d), device_id_type=MESH).start()
        r2[k, me] = s2[k, me]

    for k in range(chunks):
        span = pl.ds(0, devices - 1)
        pltpu.make_async_remote_copy(
            src_ref=r2.at[k, span], dst_ref=r2.at[k, span], send_sem=send2.at[k], recv_sem=recv2.at[k],
            device_id=(section, peer_of(1)), device_id_type=MESH).wait_recv()
        for d in range(groups):
            got = [r2[k, s * groups + d].astype(jnp.float32) for s in range(sections)]
            lane = d * width + k * LANES
            for i in range(block_len):
                out_ref[i, :, lane:lane + LANES] = jnp.concatenate(
                    [v[i * layers:(i + 1) * layers] for v in got], axis=0).astype(jnp.bfloat16)
    energy_wait.wait_send()
    for u in range(units):
        arrived(u).wait_send()
    for k in range(chunks):
        span = pl.ds(0, devices - 1)
        pltpu.make_async_remote_copy(
            src_ref=s2.at[k, span], dst_ref=r2.at[k, span], send_sem=send2.at[k], recv_sem=recv2.at[k],
            device_id=(section, peer_of(1)), device_id_type=MESH).wait_send()


def store_kernel(assembled, out_hbm, sem):
    store = pltpu.make_async_copy(assembled, out_hbm, sem)
    store.start()
    store.wait()


def solution(mesh):
    sections, groups = mesh.shape["section"], mesh.shape["dp"]

    def on_device(residuals, owners):
        layers, tokens, features = residuals.shape
        blocks = owners.shape[0]
        block_len = tokens * groups // blocks
        rows = block_len * layers
        chunks = features // groups // LANES
        early = chunks > 1
        tiles = (chunks, blocks, rows, LANES)
        part_tiles = (blocks, rows // 2, LANES)
        dma = pltpu.SemaphoreType.DMA
        received = pl.pallas_call(
            functools.partial(harvest_kernel, sections, groups, early),
            out_shape=pltpu.VMEM((block_len, layers * sections, features), jnp.bfloat16),
            in_specs=[pl.BlockSpec(memory_space=pl.ANY), pl.BlockSpec(memory_space=pl.ANY)],
            out_specs=pl.BlockSpec(memory_space=pltpu.VMEM),
            scratch_shapes=[
                pltpu.SMEM((blocks,), jnp.int32),
                pltpu.SMEM((blocks,), jnp.int32),
                pltpu.VMEM((layers, tokens, features), jnp.float32),
                pltpu.VMEM((features // LANES, blocks // groups, rows, LANES), jnp.float32),
                pltpu.VMEM((1, LANES), jnp.float32),
                pltpu.VMEM((groups, 1, LANES), jnp.float32),
                pltpu.VMEM(part_tiles, jnp.bfloat16),
                pltpu.VMEM(tiles, jnp.bfloat16),
                pltpu.VMEM(tiles, jnp.bfloat16),
                pltpu.VMEM(tiles, jnp.bfloat16),
                dma, dma, dma, dma,
                dma((chunks + early,)), dma((chunks + early,)), dma((chunks,)), dma((chunks,)),
                *([pltpu.VMEM(part_tiles, jnp.bfloat16)] if early else []),
                *[pltpu.VMEM(tiles[1:], jnp.bfloat16)] * (chunks - early),
                *([pltpu.VMEM(part_tiles, jnp.float32)] if early else []),
            ],
            compiler_params=pltpu.CompilerParams(collective_id=0, has_side_effects=True),
            name="harvest",
        )(residuals, owners)
        return pl.pallas_call(
            store_kernel,
            out_shape=jax.ShapeDtypeStruct(received.shape, received.dtype),
            in_specs=[pl.BlockSpec(memory_space=pltpu.VMEM)],
            out_specs=pl.BlockSpec(memory_space=pl.ANY),
            scratch_shapes=[pltpu.SemaphoreType.DMA],
            name="store",
        )(pltpu.with_memory_space_constraint(received, pltpu.VMEM))

    in_specs = (P("section", "dp", None), P())
    out_specs = P(("section", "dp"), None, None)
    return jax.shard_map(on_device, mesh=mesh, in_specs=in_specs, out_specs=out_specs, check_vma=False)
```

```python
import functools

import jax
import jax.numpy as jnp
from jax import lax
from jax.experimental import pallas as pl
from jax.experimental.pallas import tpu as pltpu
from jax.sharding import PartitionSpec as P

MESH = pl.DeviceIdType.MESH
LANES = 128
SUBLANES = 8


def harvest_kernel(sections, groups, early, x_hbm, owners_hbm, out_ref, owners, inverse, xv, centered, part, parts,
                   late, s1, s2, r2, x_sem, o_sem, e_send, e_recv, send1, recv1, send2, recv2, *r1):
    half = s1.shape[2] // 2
    layers, tokens, features = x_hbm.shape
    chunks, blocks, rows, _ = s1.shape
    width = features // groups
    block_len = rows // layers
    per_dev = tokens // block_len
    devices = sections * groups
    section, group = lax.axis_index("section"), lax.axis_index("dp")
    me = section * groups + group

    load = pltpu.make_async_copy(x_hbm, xv, x_sem)
    load.start()
    barrier = pltpu.get_barrier_semaphore()

    def peer_of(k):
        return lax.rem(group + k, groups)

    for k in range(1, groups):
        pl.semaphore_signal(barrier, inc=1, device_id=(section, peer_of(k)), device_id_type=MESH)
    for k in range(1, sections):
        pl.semaphore_signal(barrier, inc=1, device_id=(lax.rem(section + k, sections), group), device_id_type=MESH)

    load_owners = pltpu.make_async_copy(owners_hbm, owners, o_sem)
    load_owners.start()
    load.wait()
    per_tile = SUBLANES // layers
    lane = lax.broadcasted_iota(jnp.int32, (SUBLANES, LANES), 1)
    row = lax.broadcasted_iota(jnp.int32, (SUBLANES, LANES), 0)
    total = jnp.zeros((SUBLANES, LANES), jnp.float32)
    for l in range(layers):
        acc = jnp.zeros((SUBLANES, LANES), jnp.float32)
        for t in range(0, tokens, SUBLANES):
            x = xv[l, t:t + SUBLANES]
            c = x - jnp.sum(x, axis=1, keepdims=True) * (1.0 / features)
            xv[l, t:t + SUBLANES] = c
            sq = c * c
            for f in range(features // LANES):
                acc = acc + sq[:, f * LANES:(f + 1) * LANES]
        fold = LANES // 2
        while fold >= LANES // layers:
            acc = acc + pltpu.roll(acc, fold, 1)
            fold //= 2
        total = total + jnp.where(lane // (LANES // layers) == l, acc, 0.0)
    own_lanes = lane // (LANES // layers) == row % layers
    acc = jnp.sum(total, axis=0, keepdims=True)
    part[...] = acc
    parts[group] = acc

    pl.semaphore_wait(barrier, groups + sections - 2)
    order = sorted(range(1, groups), key=lambda p: min(p, groups - p))
    early_order = sorted(range(1, groups), key=lambda p: min(p, groups - p))
    first_order = sorted(range(1, groups), key=lambda p: min(p, groups - p))
    second_order = list(range(1, groups))
    for k in order:
        pltpu.make_async_remote_copy(
            src_ref=part, dst_ref=parts.at[group], send_sem=e_send, recv_sem=e_recv,
            device_id=(section, peer_of(k)), device_id_type=MESH).start()

    mine = pl.ds(group * per_dev, per_dev)
    units = len(r1)

    def spread(u, source):
        for p in (early_order if u == chunks else first_order):
            d = peer_of(p)
            pltpu.make_async_remote_copy(
                src_ref=source(d), dst_ref=r1[u].at[mine], send_sem=send1.at[u], recv_sem=recv1.at[u],
                device_id=(section, d), device_id_type=MESH).start()
        r1[u][mine] = source(group)[...]

    def regroup(g):
        j, r = divmod(g * SUBLANES, rows)
        c = jnp.concatenate([xv[:, g * per_tile + i, :] for i in range(per_tile)], axis=0)
        for f in range(features // LANES):
            centered[f, j, r:r + SUBLANES] = c[:, f * LANES:(f + 1) * LANES]

    tiles = range(tokens // per_tile)
    first = [g for g in tiles if g * SUBLANES % rows < half]
    for g in first:
        regroup(g)
    if early:
        spread(chunks, lambda d: centered.at[d * chunks, :, pl.ds(0, half)])

    for g in tiles:
        if g not in first:
            regroup(g)
    load_owners.wait()

    @pl.loop(0, blocks)
    def _(o):
        found = jnp.int32(0)
        for b in range(blocks):
            found = jnp.where(owners[b] == o, jnp.int32(b), found)
        inverse[o] = found

    others = pl.ds(0, groups - 1)
    energy_wait = pltpu.make_async_remote_copy(
        src_ref=parts.at[others], dst_ref=parts.at[others], send_sem=e_send, recv_sem=e_recv,
        device_id=(section, peer_of(1)), device_id_type=MESH)
    energy_wait.wait_recv()
    total = parts[0]
    for g in range(1, groups):
        total = total + parts[g]
    energy = jnp.sum(jnp.where(own_lanes, total, 0.0), axis=1, keepdims=True)
    scale = 1.0 / jnp.sqrt(energy * (1.0 / (tokens * groups * features)) + 1.0)
    scale = jnp.concatenate([scale] * (rows // SUBLANES), axis=0)

    for k in range(chunks):
        top = half if early and k == 0 else 0
        for d in range(groups):
            for j in range(per_dev):
                b = d * per_dev + j
                if top:
                    late[b] = (centered[d * chunks, j, top:] * scale[top:]).astype(jnp.bfloat16)
                else:
                    s1[k, b] = (centered[d * chunks + k, j] * scale).astype(jnp.bfloat16)
        if top:
            spread(k, lambda d: late.at[pl.ds(d * per_dev, per_dev)])
        else:
            spread(k, lambda d: s1.at[k, pl.ds(d * per_dev, per_dev)])

    def arrived(u):
        span = pl.ds(0, (groups - 1) * per_dev)
        return pltpu.make_async_remote_copy(
            src_ref=r1[u].at[span], dst_ref=r1[u].at[span], send_sem=send1.at[u], recv_sem=recv1.at[u],
            device_id=(section, peer_of(1)), device_id_type=MESH)

    def deliver(u, view):
        for p, q in [(p, q) for p in second_order + [0] for q in range(sections) if p or q]:
            sec, d = lax.rem(section + q, sections), peer_of(p)
            pltpu.make_async_remote_copy(
                src_ref=view(s2, sec * groups + d), dst_ref=view(r2, me), send_sem=send2.at[u], recv_sem=recv2.at[u],
                device_id=(sec, d), device_id_type=MESH).start()
        view(r2, me)[...] = view(s2, me)[...]

    def view_of(u):
        if u == chunks:
            return lambda ref, at: ref.at[0, at, pl.ds(0, half)]
        if early and u == 0:
            return lambda ref, at: ref.at[0, at, pl.ds(half, half)]
        return lambda ref, at: ref.at[u, at]

    def delivered(u):
        ref = view_of(u)(r2, pl.ds(0, devices - 1))
        return pltpu.make_async_remote_copy(
            src_ref=ref, dst_ref=ref, send_sem=send2.at[u], recv_sem=recv2.at[u],
            device_id=(section, peer_of(1)), device_id_type=MESH)

    for u in ([chunks] if early else []) + list(range(chunks)):
        arrived(u).wait_recv()
        for o in range(devices):
            block = r1[u][inverse[o]]
            if u == chunks:
                block = (block * scale[:half]).astype(jnp.bfloat16)
            view_of(u)(s2, o)[...] = block
        deliver(u, view_of(u))

    for k in range(chunks):
        delivered(k).wait_recv()
        if early and k == 0:
            delivered(chunks).wait_recv()
        for d in range(groups):
            got = [r2[k, s * groups + d].astype(jnp.float32) for s in range(sections)]
            lane = d * width + k * LANES
            for i in range(block_len):
                out_ref[i, :, lane:lane + LANES] = jnp.concatenate(
                    [v[i * layers:(i + 1) * layers] for v in got], axis=0).astype(jnp.bfloat16)
    energy_wait.wait_send()
    for u in range(units):
        arrived(u).wait_send()
        delivered(u).wait_send()


def store_kernel(assembled, out_hbm, sem):
    store = pltpu.make_async_copy(assembled, out_hbm, sem)
    store.start()
    store.wait()


def solution(mesh):
    sections, groups = mesh.shape["section"], mesh.shape["dp"]

    def on_device(residuals, owners):
        layers, tokens, features = residuals.shape
        blocks = owners.shape[0]
        block_len = tokens * groups // blocks
        rows = block_len * layers
        chunks = features // groups // LANES
        early = chunks > 1
        tiles = (chunks, blocks, rows, LANES)
        part_tiles = (blocks, rows // 2, LANES)
        dma = pltpu.SemaphoreType.DMA
        received = pl.pallas_call(
            functools.partial(harvest_kernel, sections, groups, early),
            out_shape=pltpu.VMEM((block_len, layers * sections, features), jnp.bfloat16),
            in_specs=[pl.BlockSpec(memory_space=pl.ANY), pl.BlockSpec(memory_space=pl.ANY)],
            out_specs=pl.BlockSpec(memory_space=pltpu.VMEM),
            scratch_shapes=[
                pltpu.SMEM((blocks,), jnp.int32),
                pltpu.SMEM((blocks,), jnp.int32),
                pltpu.VMEM((layers, tokens, features), jnp.float32),
                pltpu.VMEM((features // LANES, blocks // groups, rows, LANES), jnp.float32),
                pltpu.VMEM((1, LANES), jnp.float32),
                pltpu.VMEM((groups, 1, LANES), jnp.float32),
                pltpu.VMEM(part_tiles, jnp.bfloat16),
                pltpu.VMEM(tiles, jnp.bfloat16),
                pltpu.VMEM(tiles, jnp.bfloat16),
                pltpu.VMEM(tiles, jnp.bfloat16),
                dma, dma, dma, dma,
                *[dma((chunks + early,)) for _ in range(4)],
                *([pltpu.VMEM(part_tiles, jnp.bfloat16)] if early else []),
                *[pltpu.VMEM(tiles[1:], jnp.bfloat16)] * (chunks - early),
                *([pltpu.VMEM(part_tiles, jnp.float32)] if early else []),
            ],
            compiler_params=pltpu.CompilerParams(collective_id=0, has_side_effects=True),
            name="harvest",
        )(residuals, owners)
        return pl.pallas_call(
            store_kernel,
            out_shape=jax.ShapeDtypeStruct(received.shape, received.dtype),
            in_specs=[pl.BlockSpec(memory_space=pltpu.VMEM)],
            out_specs=pl.BlockSpec(memory_space=pl.ANY),
            scratch_shapes=[pltpu.SemaphoreType.DMA],
            name="store",
        )(pltpu.with_memory_space_constraint(received, pltpu.VMEM))

    in_specs = (P("section", "dp", None), P())
    out_specs = P(("section", "dp"), None, None)
    return jax.shard_map(on_device, mesh=mesh, in_specs=in_specs, out_specs=out_specs, check_vma=False)
```

```python
import functools

import jax
import jax.numpy as jnp
from jax import lax
from jax.experimental import pallas as pl
from jax.experimental.pallas import tpu as pltpu
from jax.sharding import PartitionSpec as P

MESH = pl.DeviceIdType.MESH
LANES = 128
SUBLANES = 8


def harvest_kernel(sections, groups, early, x_hbm, owners_hbm, out_ref, owners, inverse, xv, centered, part, parts,
                   late, s1, s2, r2, x_sem, o_sem, e_send, e_recv, send1, recv1, send2, recv2, *r1):
    half = s1.shape[2] // 2
    layers, tokens, features = x_hbm.shape
    chunks, blocks, rows, _ = s1.shape
    width = features // groups
    block_len = rows // layers
    per_dev = tokens // block_len
    devices = sections * groups
    section, group = lax.axis_index("section"), lax.axis_index("dp")
    me = section * groups + group

    load = pltpu.make_async_copy(x_hbm, xv, x_sem)
    load.start()
    barrier = pltpu.get_barrier_semaphore()

    def peer_of(k):
        return lax.rem(group + k, groups)

    for k in range(1, groups):
        pl.semaphore_signal(barrier, inc=1, device_id=(section, peer_of(k)), device_id_type=MESH)
    for k in range(1, sections):
        pl.semaphore_signal(barrier, inc=1, device_id=(lax.rem(section + k, sections), group), device_id_type=MESH)

    load_owners = pltpu.make_async_copy(owners_hbm, owners, o_sem)
    load_owners.start()
    load.wait()
    per_tile = SUBLANES // layers
    lane = lax.broadcasted_iota(jnp.int32, (SUBLANES, LANES), 1)
    row = lax.broadcasted_iota(jnp.int32, (SUBLANES, LANES), 0)
    total = jnp.zeros((SUBLANES, LANES), jnp.float32)
    for l in range(layers):
        acc = jnp.zeros((SUBLANES, LANES), jnp.float32)
        for t in range(0, tokens, SUBLANES):
            x = xv[l, t:t + SUBLANES]
            c = x - jnp.sum(x, axis=1, keepdims=True) * (1.0 / features)
            xv[l, t:t + SUBLANES] = c
            sq = c * c
            for f in range(features // LANES):
                acc = acc + sq[:, f * LANES:(f + 1) * LANES]
        fold = LANES // 2
        while fold >= LANES // layers:
            acc = acc + pltpu.roll(acc, fold, 1)
            fold //= 2
        total = total + jnp.where(lane // (LANES // layers) == l, acc, 0.0)
    own_lanes = lane // (LANES // layers) == row % layers
    acc = jnp.sum(total, axis=0, keepdims=True)
    part[...] = acc
    parts[group] = acc

    pl.semaphore_wait(barrier, groups + sections - 2)
    order = sorted(range(1, groups), key=lambda p: min(p, groups - p))
    early_order = sorted(range(1, groups), key=lambda p: min(p, groups - p))
    first_order = sorted(range(1, groups), key=lambda p: min(p, groups - p))
    second_order = list(range(1, groups))
    for k in order:
        pltpu.make_async_remote_copy(
            src_ref=part, dst_ref=parts.at[group], send_sem=e_send, recv_sem=e_recv,
            device_id=(section, peer_of(k)), device_id_type=MESH).start()

    mine = pl.ds(group * per_dev, per_dev)
    units = len(r1)

    def spread(u, source):
        for p in (early_order if u == chunks else first_order):
            d = peer_of(p)
            pltpu.make_async_remote_copy(
                src_ref=source(d), dst_ref=r1[u].at[mine], send_sem=send1.at[u], recv_sem=recv1.at[u],
                device_id=(section, d), device_id_type=MESH).start()
        r1[u][mine] = source(group)[...]

    def regroup(g):
        j, r = divmod(g * SUBLANES, rows)
        c = jnp.concatenate([xv[:, g * per_tile + i, :] for i in range(per_tile)], axis=0)
        for f in range(features // LANES):
            centered[f, j, r:r + SUBLANES] = c[:, f * LANES:(f + 1) * LANES]

    tiles = range(tokens // per_tile)
    first = [g for g in tiles if g * SUBLANES % rows < half]
    for g in first:
        regroup(g)
    if early:
        spread(chunks, lambda d: centered.at[d * chunks, :, pl.ds(0, half)])

    for g in tiles:
        if g not in first:
            regroup(g)
    load_owners.wait()

    @pl.loop(0, blocks)
    def _(o):
        found = jnp.int32(0)
        for b in range(blocks):
            found = jnp.where(owners[b] == o, jnp.int32(b), found)
        inverse[o] = found

    others = pl.ds(0, groups - 1)
    energy_wait = pltpu.make_async_remote_copy(
        src_ref=parts.at[others], dst_ref=parts.at[others], send_sem=e_send, recv_sem=e_recv,
        device_id=(section, peer_of(1)), device_id_type=MESH)
    energy_wait.wait_recv()
    total = parts[0]
    for g in range(1, groups):
        total = total + parts[g]
    energy = jnp.sum(jnp.where(own_lanes, total, 0.0), axis=1, keepdims=True)
    scale = 1.0 / jnp.sqrt(energy * (1.0 / (tokens * groups * features)) + 1.0)
    scale = jnp.concatenate([scale] * (rows // SUBLANES), axis=0)

    for k in range(chunks):
        top = half if early and k == 0 else 0
        for d in range(groups):
            for j in range(per_dev):
                b = d * per_dev + j
                if top:
                    late[b] = (centered[d * chunks, j, top:] * scale[top:]).astype(jnp.bfloat16)
                else:
                    s1[k, b] = (centered[d * chunks + k, j] * scale).astype(jnp.bfloat16)
        if top:
            spread(k, lambda d: late.at[pl.ds(d * per_dev, per_dev)])
        else:
            spread(k, lambda d: s1.at[k, pl.ds(d * per_dev, per_dev)])

    def arrived(u):
        span = pl.ds(0, (groups - 1) * per_dev)
        return pltpu.make_async_remote_copy(
            src_ref=r1[u].at[span], dst_ref=r1[u].at[span], send_sem=send1.at[u], recv_sem=recv1.at[u],
            device_id=(section, peer_of(1)), device_id_type=MESH)

    routes = [(p, q) for p in second_order + [0] for q in range(sections)]
    lag = 8

    def deliver(u, view):
        def place(p, q):
            sec, d = lax.rem(section + q, sections), peer_of(p)
            return sec, d, sec * groups + d

        def select(p, q):
            o = place(p, q)[2]
            block = r1[u][inverse[o]]
            if u == chunks:
                block = (block * scale[:half]).astype(jnp.bfloat16)
            view(s2 if p or q else r2, o)[...] = block

        def send(p, q):
            if p or q:
                sec, d, o = place(p, q)
                pltpu.make_async_remote_copy(
                    src_ref=view(s2, o), dst_ref=view(r2, me), send_sem=send2.at[u], recv_sem=recv2.at[u],
                    device_id=(sec, d), device_id_type=MESH).start()

        for n in range(len(routes) + lag):
            if n < len(routes):
                select(*routes[n])
            if n >= lag:
                send(*routes[n - lag])

    def view_of(u):
        if u == chunks:
            return lambda ref, at: ref.at[0, at, pl.ds(0, half)]
        if early and u == 0:
            return lambda ref, at: ref.at[0, at, pl.ds(half, half)]
        return lambda ref, at: ref.at[u, at]

    def delivered(u):
        ref = view_of(u)(r2, pl.ds(0, devices - 1))
        return pltpu.make_async_remote_copy(
            src_ref=ref, dst_ref=ref, send_sem=send2.at[u], recv_sem=recv2.at[u],
            device_id=(section, peer_of(1)), device_id_type=MESH)

    for u in ([chunks] if early else []) + list(range(chunks)):
        arrived(u).wait_recv()
        deliver(u, view_of(u))

    for k in range(chunks):
        delivered(k).wait_recv()
        if early and k == 0:
            delivered(chunks).wait_recv()
        for d in range(groups):
            got = [r2[k, s * groups + d].astype(jnp.float32) for s in range(sections)]
            lane = d * width + k * LANES
            for i in range(block_len):
                out_ref[i, :, lane:lane + LANES] = jnp.concatenate(
                    [v[i * layers:(i + 1) * layers] for v in got], axis=0).astype(jnp.bfloat16)
    energy_wait.wait_send()
    for u in range(units):
        arrived(u).wait_send()
        delivered(u).wait_send()


def store_kernel(assembled, out_hbm, sem):
    store = pltpu.make_async_copy(assembled, out_hbm, sem)
    store.start()
    store.wait()


def solution(mesh):
    sections, groups = mesh.shape["section"], mesh.shape["dp"]

    def on_device(residuals, owners):
        layers, tokens, features = residuals.shape
        blocks = owners.shape[0]
        block_len = tokens * groups // blocks
        rows = block_len * layers
        chunks = features // groups // LANES
        early = chunks > 1
        tiles = (chunks, blocks, rows, LANES)
        part_tiles = (blocks, rows // 2, LANES)
        dma = pltpu.SemaphoreType.DMA
        received = pl.pallas_call(
            functools.partial(harvest_kernel, sections, groups, early),
            out_shape=pltpu.VMEM((block_len, layers * sections, features), jnp.bfloat16),
            in_specs=[pl.BlockSpec(memory_space=pl.ANY), pl.BlockSpec(memory_space=pl.ANY)],
            out_specs=pl.BlockSpec(memory_space=pltpu.VMEM),
            scratch_shapes=[
                pltpu.SMEM((blocks,), jnp.int32),
                pltpu.SMEM((blocks,), jnp.int32),
                pltpu.VMEM((layers, tokens, features), jnp.float32),
                pltpu.VMEM((features // LANES, blocks // groups, rows, LANES), jnp.float32),
                pltpu.VMEM((1, LANES), jnp.float32),
                pltpu.VMEM((groups, 1, LANES), jnp.float32),
                pltpu.VMEM(part_tiles, jnp.bfloat16),
                pltpu.VMEM(tiles, jnp.bfloat16),
                pltpu.VMEM(tiles, jnp.bfloat16),
                pltpu.VMEM(tiles, jnp.bfloat16),
                dma, dma, dma, dma,
                *[dma((chunks + early,)) for _ in range(4)],
                *([pltpu.VMEM(part_tiles, jnp.bfloat16)] if early else []),
                *[pltpu.VMEM(tiles[1:], jnp.bfloat16)] * (chunks - early),
                *([pltpu.VMEM(part_tiles, jnp.float32)] if early else []),
            ],
            compiler_params=pltpu.CompilerParams(collective_id=0, has_side_effects=True),
            name="harvest",
        )(residuals, owners)
        return pl.pallas_call(
            store_kernel,
            out_shape=jax.ShapeDtypeStruct(received.shape, received.dtype),
            in_specs=[pl.BlockSpec(memory_space=pltpu.VMEM)],
            out_specs=pl.BlockSpec(memory_space=pl.ANY),
            scratch_shapes=[pltpu.SemaphoreType.DMA],
            name="store",
        )(pltpu.with_memory_space_constraint(received, pltpu.VMEM))

    in_specs = (P("section", "dp", None), P())
    out_specs = P(("section", "dp"), None, None)
    return jax.shard_map(on_device, mesh=mesh, in_specs=in_specs, out_specs=out_specs, check_vma=False)
```
